64 devices in a mesh: rep: 8 (over x, y, core), dp: 8 (over z).
Axes of the slice: x: 2, y: 2, z: 8, core: 2. Of those that a mesh axis runs over, the one named last changes fastest.
The devices are a block of a 4x4x8 slice.
Arguments:
- x: bfloat16 [64, 4096, 512], P(('rep', 'dp')), parts along dimension 0
- dy: bfloat16 [64, 4096, 512], P(('rep', 'dp')), parts along dimension 0
- w_gate: bfloat16 [2, 512, 1280], replicated
- w_up: bfloat16 [2, 512, 1280], replicated
- w_down: bfloat16 [2, 1280, 512], replicated
- m_w_gate: float32 [2, 512, 1280], P(None, 'dp')
- m_w_up: float32 [2, 512, 1280], P(None, 'dp')
- m_w_down: float32 [2, 1280, 512], P(None, 'dp')
- v_w_gate: float32 [2, 512, 1280], P(None, 'dp')
- v_w_up: float32 [2, 512, 1280], P(None, 'dp')
- v_w_down: float32 [2, 1280, 512], P(None, 'dp')
Outputs:
- output 1: bfloat16 [16, 512, 1280], P('rep'), parts along dimension 0
- output 2: bfloat16 [16, 512, 1280], P('rep'), parts along dimension 0
- output 3: bfloat16 [16, 1280, 512], P('rep'), parts along dimension 0
- output 4: float32 [16, 512, 1280], P('rep', 'dp'), parts along dimension 0
- output 5: float32 [16, 512, 1280], P('rep', 'dp'), parts along dimension 0
- output 6: float32 [16, 1280, 512], P('rep', 'dp'), parts along dimension 0
- output 7: float32 [16, 512, 1280], P('rep', 'dp'), parts along dimension 0
- output 8: float32 [16, 512, 1280], P('rep', 'dp'), parts along dimension 0
- output 9: float32 [16, 1280, 512], P('rep', 'dp'), parts along dimension 0
There are 8 independent parts. The reference program is written for one: setup_inputs(seed, part) draws one part's arguments, and reference() takes and returns one part's arrays. A program takes and returns all parts, laid end to end along the dimension named above; an argument that names none is the same for every part.
All inputs are finite; a program needn't handle non-finite values.
Results may differ from the reference program's by a relative error of at most 0.022.
Values are sent between devices in bfloat16 or wider.
A program may use at most 768 MiB of HBM per device.

```python
import jax
import jax.numpy as jnp
from jax import lax

SEQUENCES = 8
TOKENS = 4096
D = 512
FF = 1280
LAYERS = 2
NAMES = ("w_gate", "w_up", "w_down")
SHAPES = {"w_gate": (LAYERS, D, FF), "w_up": (LAYERS, D, FF), "w_down": (LAYERS, FF, D)}


def bump(key, n, height):
    away = (jnp.arange(n, dtype=jnp.int32) - jax.random.randint(key, (), 0, n, jnp.int32)) % n
    return jnp.where(away < n // 8, height, 1.0)


def together(key, own, strength):
    shared = jax.random.normal(key, own.shape[1:], jnp.float32)
    return (own + strength * shared) * lax.rsqrt(1 + strength * strength)


def setup_inputs(seed: int = 0, part: int = 0) -> dict:
    kx, kdy, ka, kb, kz, kf, kh, kl, *keys = jax.random.split(jax.random.key(seed), 8 + 3 * len(NAMES))
    kx, kdy, ka, kb = (jax.random.fold_in(k, part) for k in (kx, kdy, ka, kb))
    kw, km, kv = (keys[i::3] for i in range(3))
    shape = (SEQUENCES, TOKENS, D)
    much_x, much_dy = jax.random.uniform(kz, (2,), jnp.float32, 0.0, 1.0)
    loud = 2.0 ** jax.random.uniform(jax.random.fold_in(kz, 1), (), jnp.float32, -1.0, 2.0)
    layers = 2.0 ** jax.random.uniform(kl, (LAYERS, 1, 1), jnp.float32, -1.0, 1.0)
    x = together(ka, jax.random.normal(kx, shape, jnp.float32), much_x) * bump(kf, D, 4.0)
    dy = together(kb, jax.random.normal(kdy, shape, jnp.float32), much_dy)
    drawn = {"x": x.astype(jnp.bfloat16), "dy": (loud * dy * (SEQUENCES * TOKENS) ** -0.5).astype(jnp.bfloat16)}
    for key, name in zip(kw, NAMES, strict=True):
        w = jax.random.normal(key, SHAPES[name], jnp.float32) * SHAPES[name][1] ** -0.5
        drawn[name] = (w * {"w_gate": 1.0, "w_up": bump(kh, FF, 4.0), "w_down": layers}[name]).astype(jnp.bfloat16)
    for key, name in zip(km, NAMES, strict=True):
        drawn[f"m_{name}"] = 0.1 * jax.random.normal(key, SHAPES[name], jnp.float32)
    for key, name in zip(kv, NAMES, strict=True):
        drawn[f"v_{name}"] = jax.random.uniform(key, SHAPES[name], jnp.float32, 0.005, 0.015)
    return drawn


def matmul(a, w):
    return jnp.dot(a, w, preferred_element_type=jnp.float32).astype(jnp.bfloat16)


def normed(h):
    wide = h.astype(jnp.float32)
    scale = lax.rsqrt(jnp.mean(wide**2, -1, keepdims=True) + 1e-6)
    return (wide * scale).astype(jnp.bfloat16)


def layer(h, w):
    a = normed(h)
    gate = jnp.dot(a, w["w_gate"], preferred_element_type=jnp.float32)
    up = jnp.dot(a, w["w_up"], preferred_element_type=jnp.float32)
    return h + matmul((jax.nn.silu(gate) * up).astype(jnp.bfloat16), w["w_down"])


def adamw(w, m, v, g):
    m = 0.9 * m + 0.1 * g
    v = 0.95 * v + 0.05 * g * g
    step = m * lax.rsqrt(v + 1e-8) + 0.1 * w
    return (w - 0.02 * step).astype(jnp.bfloat16), m, v


def clipped(gradients, sum_of_squares, count):
    factor = jnp.minimum(1.0, 0.5 * lax.rsqrt(sum_of_squares / count + 1e-30))
    return [g * factor for g in gradients]


def stack(weights, h):
    return lax.scan(lambda h, w: (layer(h, w), None), h, weights)[0]


def reference(x, dy, w_gate, w_up, w_down, m_w_gate, m_w_up, m_w_down, v_w_gate, v_w_up, v_w_down):
    weights = dict(zip(NAMES, (w_gate, w_up, w_down), strict=True))

    def take(so_far, sequence):
        h, by_y = sequence
        _, back = jax.vjp(lambda w: stack(w, h), weights)
        return jax.tree.map(lambda total, term: total + term.astype(jnp.float32), so_far, back(by_y)[0]), None

    none_yet = {name: jnp.zeros(w.shape, jnp.float32) for name, w in weights.items()}
    by_weights, _ = lax.scan(take, none_yet, (x, dy))
    gradients = [by_weights[name].astype(jnp.bfloat16).astype(jnp.float32) for name in NAMES]
    gradients = clipped(gradients, sum(jnp.sum(g * g) for g in gradients), sum(g.size for g in gradients))
    new = [
        adamw(w.astype(jnp.float32), m, v, g)
        for w, m, v, g in zip((w_gate, w_up, w_down), (m_w_gate, m_w_up, m_w_down), (v_w_gate, v_w_up, v_w_down), gradients, strict=True)
    ]
    return tuple(one[which] for which in range(3) for one in new)
```

```python
import functools

import jax
import jax.numpy as jnp
from jax import lax
from jax.experimental import pallas as pl
from jax.experimental.pallas import tpu as pltpu
from jax.sharding import PartitionSpec as P

BF16, F32 = jnp.bfloat16, jnp.float32
FB = 256
TF = 512
TB = 1024


def dot(a, b):
    return jnp.dot(a, b, preferred_element_type=F32)


def dot_nt(a, b):
    return lax.dot_general(a, b, (((1,), (1,)), ((), ())), preferred_element_type=F32)


def scale_of(wide):
    return lax.rsqrt(jnp.mean(wide * wide, -1, keepdims=True) + 1e-6)


def sigmoid(g):
    return 0.5 * jnp.tanh(0.5 * g) + 0.5


def forward(x, dy, w, h, a2, a_t, dy_t, hid):
    wg, wu, wd = w
    blocks = wg.shape[2] // FB

    def tile(i, _):
        rows = pl.ds(pl.multiple_of(i * TF, TF), TF)
        wide = x[rows, :].astype(F32)
        a = (wide * scale_of(wide)).astype(BF16)
        for j in range(blocks):
            cols = pl.ds(j * FB, FB)
            gate, up = dot(a, wg[0, :, cols]), dot(a, wu[0, :, cols])
            hid[:, cols] = (gate * sigmoid(gate) * up).astype(BF16)
        out = dot(hid[...], wd[0]).astype(BF16).astype(F32)
        state = (wide + out).astype(BF16)
        h[rows, :] = state
        wide = state.astype(F32)
        n = (wide * scale_of(wide)).astype(BF16)
        a2[rows, :] = n
        a_t[:, rows] = n.T
        dy_t[:, rows] = dy[rows, :].T
        x[rows, :] = a
        return 0

    lax.fori_loop(0, x.shape[0] // TF, tile, 0)


def backward_tile(layer, j, i, a_ref, a_t, dy, dy_t, w, acc, da):
    wg, wu, wd = w
    rows = pl.ds(pl.multiple_of(i * TB, TB), TB)
    cols = pl.ds(pl.multiple_of(j * FB, FB), FB)
    acc_g, acc_u, acc_d = acc
    hids, dgates, dups = [], [], []
    half = TB // 2
    for s in range(2):
        sub = pl.ds(pl.multiple_of(i * TB + s * half, half), half)
        a = a_ref[sub, :]
        gate, up = dot(a, wg[layer, :, cols]), dot(a, wu[layer, :, cols])
        dh = dot_nt(dy[sub, :], wd[layer, cols, :]).astype(BF16).astype(F32)
        sg = sigmoid(gate)
        silu = gate * sg
        hids.append((silu * up).astype(BF16))
        dups.append((dh * silu).astype(BF16))
        dgates.append((dh * up * (sg + silu * (1.0 - sg))).astype(BF16))
        if da is not None:
            term = dot_nt(dgates[s], wg[layer, :, cols]) + dot_nt(dups[s], wu[layer, :, cols])

            @pl.when(j == 0)
            def _(sub=sub, term=term):
                da[sub, :] = term

            @pl.when(j > 0)
            def _(sub=sub, term=term):
                da[sub, :] += term

    hid, dgate, dup = (jnp.concatenate(t, 0) for t in (hids, dgates, dups))
    terms = dot(a_t[:, rows], dgate), dot(a_t[:, rows], dup), dot(dy_t[:, rows], hid)

    @pl.when(i == 0)
    def _():
        for to, term in zip(acc, terms, strict=True):
            to[...] = term

    @pl.when(i > 0)
    def _():
        for to, term in zip(acc, terms, strict=True):
            to[...] += term


def backward(layer, a_ref, a_t, dy, dy_t, w, acc, da, grads):
    steps = dy.shape[0] // TB
    gg, gu, gd = grads

    def block(j, _):
        def tile(i, _):
            backward_tile(layer, j, i, a_ref, a_t, dy, dy_t, w, acc, da)
            return 0

        lax.fori_loop(0, steps, tile, 0)
        cols = pl.ds(pl.multiple_of(j * FB, FB), FB)
        gg[layer, :, cols] = acc[0][...].astype(BF16)
        gu[layer, :, cols] = acc[1][...].astype(BF16)
        gd[layer, cols, :] = acc[2][...].astype(BF16).T
        return 0

    lax.fori_loop(0, w[0].shape[2] // FB, block, 0)


def between(a1, h, dy, a_t, dy_t, da):
    def tile(i, _):
        rows = pl.ds(pl.multiple_of(i * TF, TF), TF)
        wide = h[rows, :].astype(F32)
        by_a = da[rows, :].astype(BF16).astype(F32)
        scale = scale_of(wide)
        inner = jnp.mean(by_a * wide, -1, keepdims=True)
        by_h = scale * by_a - wide * (scale * scale * scale * inner)
        total = (dy[rows, :].astype(F32) + by_h.astype(BF16).astype(F32)).astype(BF16)
        dy[rows, :] = total
        dy_t[:, rows] = total.T
        a_t[:, rows] = a1[rows, :].T
        return 0

    lax.fori_loop(0, h.shape[0] // TF, tile, 0)


def kernel(x_in, dy_in, wg_in, wu_in, wd_in, gg, gu, gd, x, dy, wg, wu, wd, h, a2, a_t, dy_t, hid, da, ag, au, ad, sems):
    copies = [
        pltpu.make_async_copy(src, dst, sems.at[k])
        for k, (src, dst) in enumerate(((x_in.at[0], x), (dy_in.at[0], dy), (wg_in, wg), (wu_in, wu), (wd_in, wd)))
    ]
    for c in copies:
        c.start()
    for c in copies:
        c.wait()
    w, acc, grads = (wg, wu, wd), (ag, au, ad), (gg, gu, gd)
    forward(x, dy, w, h, a2, a_t, dy_t, hid)
    backward(1, a2, a_t, dy, dy_t, w, acc, da, grads)
    between(x, h, dy, a_t, dy_t, da)
    backward(0, x, a_t, dy, dy_t, w, acc, None, grads)


def gradients(x, dy, wg, wu, wd):
    _, t, d = x.shape
    ff = wg.shape[2]
    any_, vm = pl.BlockSpec(memory_space=pl.ANY), pl.BlockSpec(memory_space=pltpu.VMEM)
    return pl.pallas_call(
        kernel,
        out_shape=[jax.ShapeDtypeStruct(w.shape, BF16) for w in (wg, wu, wd)],
        in_specs=[any_] * 5,
        out_specs=[vm] * 3,
        scratch_shapes=[
            pltpu.VMEM((t, d), BF16),
            pltpu.VMEM((t, d), BF16),
            pltpu.VMEM(wg.shape, BF16),
            pltpu.VMEM(wu.shape, BF16),
            pltpu.VMEM(wd.shape, BF16),
            pltpu.VMEM((t, d), BF16),
            pltpu.VMEM((t, d), BF16),
            pltpu.VMEM((d, t), BF16),
            pltpu.VMEM((d, t), BF16),
            pltpu.VMEM((TF, ff), BF16),
            pltpu.VMEM((t, d), F32),
            pltpu.VMEM((d, FB), F32),
            pltpu.VMEM((d, FB), F32),
            pltpu.VMEM((d, FB), F32),
            pltpu.SemaphoreType.DMA((5,)),
        ],
        compiler_params=pltpu.CompilerParams(vmem_limit_bytes=67_000_000),
        name="gradients",
    )(x, dy, wg, wu, wd)


def solution(mesh):
    def step(x, dy, *arrays):
        weights, m, v = (arrays[i : i + 3] for i in (0, 3, 6))
        n = lax.axis_size("dp")
        me = lax.axis_index("dp")
        terms = gradients(x, dy, *weights)
        g = [lax.psum_scatter(t, "dp", scatter_dimension=1, tiled=True).astype(F32) for t in terms]
        count = sum(w.size for w in weights)
        squares = lax.psum(sum(jnp.sum(t * t) for t in g), "dp")
        factor = jnp.minimum(1.0, 0.5 * lax.rsqrt(squares / count + 1e-30))
        new = ([], [], [])
        for w, m_, v_, t in zip(weights, m, v, g, strict=True):
            t = t * factor
            rows = w.shape[1] // n
            own = lax.dynamic_slice_in_dim(w, me * rows, rows, 1).astype(F32)
            m_ = 0.9 * m_ + 0.1 * t
            v_ = 0.95 * v_ + 0.05 * t * t
            own = (own - 0.02 * (m_ * lax.rsqrt(v_ + 1e-8) + 0.1 * own)).astype(BF16)
            new[0].append(lax.all_gather(own, "dp", axis=1, tiled=True))
            new[1].append(m_)
            new[2].append(v_)
        return tuple(t for three in new for t in three)

    seq, whole, block = P(("rep", "dp"), None, None), P(None, None, None), P(None, "dp", None)
    return jax.shard_map(
        step,
        mesh=mesh,
        in_specs=(seq, seq, *[whole] * 3, *[block] * 6),
        out_specs=(*[P("rep", None, None)] * 3, *[P("rep", "dp", None)] * 6),
        check_vma=False,
    )
```

```python
import functools

import jax
import jax.numpy as jnp
from jax import lax
from jax.experimental import pallas as pl
from jax.experimental.pallas import tpu as pltpu
from jax.sharding import PartitionSpec as P

BF16, F32 = jnp.bfloat16, jnp.float32
FB = 256
TF = 512
TB = 1024


def dot(a, b):
    return jnp.dot(a, b, preferred_element_type=F32)


def dot_nt(a, b):
    return lax.dot_general(a, b, (((1,), (1,)), ((), ())), preferred_element_type=F32)


def scale_of(wide):
    return lax.rsqrt(jnp.mean(wide * wide, -1, keepdims=True) + 1e-6)


def sigmoid(g):
    return 0.5 * jnp.tanh(0.5 * g) + 0.5


def forward(x, dy, w, h, a2, a_t, dy_t, hid):
    wg, wu, wd = w
    blocks = wg.shape[2] // FB

    def tile(i, _):
        rows = pl.ds(pl.multiple_of(i * TF, TF), TF)
        wide = x[rows, :].astype(F32)
        a = (wide * scale_of(wide)).astype(BF16)
        for j in range(blocks):
            cols = pl.ds(j * FB, FB)
            gate, up = dot(a, wg[0, :, cols]), dot(a, wu[0, :, cols])
            hid[:, cols] = (gate * sigmoid(gate) * up).astype(BF16)
        out = dot(hid[...], wd[0]).astype(BF16).astype(F32)
        state = (wide + out).astype(BF16)
        h[rows, :] = state
        wide = state.astype(F32)
        n = (wide * scale_of(wide)).astype(BF16)
        a2[rows, :] = n
        a_t[:, rows] = n.T
        dy_t[:, rows] = dy[rows, :].T
        x[rows, :] = a
        return 0

    lax.fori_loop(0, x.shape[0] // TF, tile, 0)


def backward_tile(layer, j, i, a_ref, a_t, dy, dy_t, w, acc, da):
    wg, wu, wd = w
    rows = pl.ds(pl.multiple_of(i * TB, TB), TB)
    cols = pl.ds(pl.multiple_of(j * FB, FB), FB)
    acc_g, acc_u, acc_d = acc
    hids, dgates, dups = [], [], []
    half = TB // 2
    for s in range(2):
        sub = pl.ds(pl.multiple_of(i * TB + s * half, half), half)
        a = a_ref[sub, :]
        gate, up = dot(a, wg[layer, :, cols]), dot(a, wu[layer, :, cols])
        dh = dot_nt(dy[sub, :], wd[layer, cols, :]).astype(BF16).astype(F32)
        sg = sigmoid(gate)
        silu = gate * sg
        hids.append((silu * up).astype(BF16))
        dups.append((dh * silu).astype(BF16))
        dgates.append((dh * up * (sg + silu * (1.0 - sg))).astype(BF16))
        if da is not None:
            term = dot_nt(dgates[s], wg[layer, :, cols]) + dot_nt(dups[s], wu[layer, :, cols])

            @pl.when(j == 0)
            def _(sub=sub, term=term):
                da[sub, :] = term

            @pl.when(j > 0)
            def _(sub=sub, term=term):
                da[sub, :] += term

    hid, dgate, dup = (jnp.concatenate(t, 0) for t in (hids, dgates, dups))
    terms = dot(a_t[:, rows], dgate), dot(a_t[:, rows], dup), dot(dy_t[:, rows], hid)

    @pl.when(i == 0)
    def _():
        for to, term in zip(acc, terms, strict=True):
            to[...] = term

    @pl.when(i > 0)
    def _():
        for to, term in zip(acc, terms, strict=True):
            to[...] += term


def between(a1, h, dy, a_t, dy_t, da):
    def tile(i, _):
        rows = pl.ds(pl.multiple_of(i * TF, TF), TF)
        wide = h[rows, :].astype(F32)
        by_a = da[rows, :].astype(BF16).astype(F32)
        scale = scale_of(wide)
        inner = jnp.mean(by_a * wide, -1, keepdims=True)
        by_h = scale * by_a - wide * (scale * scale * scale * inner)
        total = (dy[rows, :].astype(F32) + by_h.astype(BF16).astype(F32)).astype(BF16)
        dy[rows, :] = total
        dy_t[:, rows] = total.T
        a_t[:, rows] = a1[rows, :].T
        return 0

    lax.fori_loop(0, h.shape[0] // TF, tile, 0)


def exchanged(me, n):
    return lax.rem(me + 1, n), lax.rem(me + n - 1, n)


def remote(src, dst, send, recv, to):
    return pltpu.make_async_remote_copy(
        src_ref=src, dst_ref=dst, send_sem=send, recv_sem=recv, device_id={"dp": to}, device_id_type=pl.DeviceIdType.MESH
    )


class Ring:
    def __init__(self, terms, slots, send, recv, rows, me, n):
        self.terms, self.slots, self.send, self.recv, self.rows, self.me, self.n = terms, slots, send, recv, rows, me, n

    def chunk(self, way, hop):
        at = lax.rem(self.me + self.n - 1 - hop, self.n) if way == 0 else lax.rem(self.me + 1 + hop, self.n)
        return pl.ds(pl.multiple_of(at * self.rows[0], self.rows[2]) + self.rows[1], self.rows[2])

    def copy(self, way, hop):
        return remote(
            self.terms[way].at[self.chunk(way, hop), :],
            self.slots[way].at[hop],
            self.send.at[way, hop],
            self.recv.at[way, hop],
            exchanged(self.me, self.n)[way],
        )

    def begin(self):
        for way in range(2):
            self.copy(way, 0).start()

    def add(self, hop):
        for way in range(2):
            self.copy(way, hop - 1).wait()
        for way in range(2):
            at = self.chunk(way, hop)
            own = self.terms[way][at, :].astype(F32)
            self.terms[way][at, :] = (own + self.slots[way][hop - 1].astype(F32)).astype(BF16)

    def go_on(self, hop):
        for way in range(2):
            self.copy(way, hop).start()


def kernel(n, x_in, dy_in, wg_in, wu_in, wd_in, mg_in, mu_in, md_in, vg_in, vu_in, vd_in,
           og, ou, od, mg_out, mu_out, md_out, vg_out, vu_out, vd_out,
           x, dy, wg, wu, wd, h, a2, a_t, dy_t, hid, da, ag, au, ad,
           tg, tu, td, slot_g, slot_u, slot_d, mg, mu, md, vg, vu, vd, ng, nu, nd, mine, others,
           sems, msems, rs_send, rs_recv, rd_send, rd_recv, sq_send, sq_recv, ag_send, ag_recv, osems):
    me = lax.axis_index("dp")
    layers, d, ff = wg.shape
    blocks = ff // FB
    ticks = n // 2
    pieces = layers * blocks
    copies = [
        pltpu.make_async_copy(src, dst, sems.at[k])
        for k, (src, dst) in enumerate(((x_in.at[0], x), (dy_in.at[0], dy), (wg_in, wg), (wu_in, wu), (wd_in, wd)))
    ]
    moments = (mg, mu, md, vg, vu, vd)
    later = [
        pltpu.make_async_copy(src, dst, msems.at[k])
        for k, (src, dst) in enumerate(zip((mg_in, mu_in, md_in, vg_in, vu_in, vd_in), moments, strict=True))
    ]
    for c in copies + later:
        c.start()
    barrier = pltpu.get_barrier_semaphore()
    for off in range(1, n):
        pl.semaphore_signal(barrier, 1, device_id={"dp": lax.rem(me + off, n)}, device_id_type=pl.DeviceIdType.MESH)
    pl.semaphore_wait(barrier, n - 1)
    for c in copies:
        c.wait()
    w, acc = (wg, wu, wd), (ag, au, ad)
    forward(x, dy, w, h, a2, a_t, dy_t, hid)

    per, per_d = d // n, ff // n
    half = per_d // 2

    def ring(p):
        s = lax.rem(p, 3)
        return Ring((tg.at[p], tu.at[p]), (slot_g.at[s], slot_u.at[s]), rs_send.at[s], rs_recv.at[s], (per, 0, per), me, n)

    def ring_d(layer, part):
        k = layer * 2 + part
        terms = tuple(td.at[layer, way] for way in range(2))
        slots = tuple(slot_d.at[k, way] for way in range(2))
        return Ring(terms, slots, rd_send.at[k], rd_recv.at[k], (per_d, part * half, half), me, n)

    def tick(p, i):
        @pl.when(jnp.logical_and(p >= 2, p < pieces + 2))
        def _():
            old = ring(p - 2)
            old.add(i + ticks)

            @pl.when(i < ticks - 1)
            def _():
                old.go_on(i + ticks)

        @pl.when(jnp.logical_and(p >= 1, p < pieces + 1))
        def _():
            new = ring(p - 1)

            @pl.when(i > 0)
            def _():
                new.add(i)

            new.go_on(i)

    def tick_d(layer, step):
        @pl.when(step == 0)
        def _():
            for part in range(2):
                ring_d(layer, part).begin()

        @pl.when(jnp.logical_and(step > 0, step < n))
        def _():
            for part in range(2):
                one = ring_d(layer, part)
                one.add(step)

                @pl.when(step < n - 1)
                def _(one=one):
                    one.go_on(step)

    def backward(layer, first, a_ref, da):
        def block(j, _):
            p = first + j

            def tile(i, _):
                tick(p, i)
                if first:
                    k = j * ticks + i

                    @pl.when(lax.rem(k, 2) == 0)
                    def _():
                        tick_d(1, k // 2)

                backward_tile(layer, j, i, a_ref, a_t, dy, dy_t, w, acc, da)
                return 0

            lax.fori_loop(0, ticks, tile, 0)
            tg[p] = ag[...].astype(BF16)
            tu[p] = au[...].astype(BF16)
            rows = pl.ds(pl.multiple_of(j * FB, FB), FB)
            by_down = ad[...].astype(BF16).T
            td[layer, 0, rows, :] = by_down[:, : d // 2]
            td[layer, 1, rows, :] = by_down[:, d // 2 :]
            return 0

        lax.fori_loop(0, blocks, block, 0)

    backward(1, 0, a2, da)
    between(x, h, dy, a_t, dy_t, da)
    backward(0, blocks, x, None)

    def drain(k, _):
        tick(pieces + k // ticks, lax.rem(k, ticks))
        tick_d(0, k)
        return 0

    lax.fori_loop(0, n, drain, 0)

    own, own_d = pl.ds(pl.multiple_of(me * per, per), per), pl.ds(pl.multiple_of(me * per_d, per_d), per_d)
    total = jnp.zeros((8, 128), F32)

    def squares(t):
        t = t.astype(F32)
        return jnp.sum(t * t)

    local = jnp.float32(0)
    for p in range(pieces):
        local += squares(tg[p, own, :]) + squares(tu[p, own, :])
    for layer in range(layers):
        for way in range(2):
            local += squares(td[layer, way, own_d, :])
    mine[...] = total + local
    sent = [remote(mine, others.at[k - 1], sq_send.at[k - 1], sq_recv.at[k - 1], lax.rem(me + k, n)) for k in range(1, n)]
    for c in sent:
        c.start()
    for c in later:
        c.wait()
    for c in sent:
        c.wait()
    summed = mine[...]
    for k in range(n - 1):
        summed = summed + others[k]
    count = layers * d * ff * 3
    factor = jnp.minimum(1.0, 0.5 * lax.rsqrt(summed[0:1, 0:1] / count + 1e-30))

    def adamw(w_own, m_at, v_at, g, new):
        g = g.astype(F32) * factor
        m_ = 0.9 * m_at[...] + 0.1 * g
        v_ = 0.95 * v_at[...] + 0.05 * g * g
        m_at[...] = m_
        v_at[...] = v_
        w_own = w_own.astype(F32)
        new[...] = (w_own - 0.02 * (m_ * lax.rsqrt(v_ + 1e-8) + 0.1 * w_own)).astype(BF16)

    outs, news, owns = (og, ou, od), (ng, nu, nd), (own, own, own_d)

    def gather(kind, way, hop):
        layer = way
        at = lax.rem(me + n - hop, n) if way == 0 else lax.rem(me + hop, n)
        size = per_d if kind == 2 else per
        rows = outs[kind].at[layer, pl.ds(pl.multiple_of(at * size, size), size), :]
        src = news[kind].at[layer] if isinstance(hop, int) and hop == 0 else rows
        return remote(src, rows, ag_send.at[way, hop, kind], ag_recv.at[way, hop, kind], exchanged(me, n)[way])

    finals = []
    for kind in range(3):
        for layer in range(layers):
            if kind < 2:
                for j in range(blocks):
                    cols = pl.ds(j * FB, FB)
                    adamw(
                        w[kind][layer, own, cols],
                        (mg, mu)[kind].at[layer, :, cols],
                        (vg, vu)[kind].at[layer, :, cols],
                        (tg, tu)[kind][(layers - 1 - layer) * blocks + j, own, :],
                        news[kind].at[layer, :, cols],
                    )
            else:
                for way in range(2):
                    cols = pl.ds(way * (d // 2), d // 2)
                    adamw(wd[layer, own_d, cols], md.at[layer, :, cols], vd.at[layer, :, cols], td[layer, way, own_d, :], nd.at[layer, :, cols])
            gather(kind, layer, 0).start()
        finals.append(pltpu.make_async_copy(news[kind], outs[kind].at[:, owns[kind], :], osems.at[kind]))
        finals.append(pltpu.make_async_copy(moments[kind], (mg_out, mu_out, md_out)[kind], osems.at[3 + kind]))
        finals.append(pltpu.make_async_copy(moments[3 + kind], (vg_out, vu_out, vd_out)[kind], osems.at[6 + kind]))
        for c in finals[-3:]:
            c.start()
    for hop in range(1, n):
        for kind in range(3):
            for way in range(2):
                gather(kind, way, hop - 1).wait()
                if hop < n - 1:
                    gather(kind, way, hop).start()
    for c in finals:
        c.wait()


def stepped(n, x, dy, *arrays):
    _, t, d = x.shape
    wg, _, wd = arrays[:3]
    layers, _, ff = wg.shape
    per, per_d = d // n, ff // n
    pieces = layers * (ff // FB)
    any_ = pl.BlockSpec(memory_space=pl.ANY)
    dma = pltpu.SemaphoreType.DMA
    return pl.pallas_call(
        functools.partial(kernel, n),
        out_shape=[jax.ShapeDtypeStruct(a.shape, a.dtype) for a in arrays],
        in_specs=[any_] * 11,
        out_specs=[any_] * 9,
        scratch_shapes=[
            pltpu.VMEM((t, d), BF16),
            pltpu.VMEM((t, d), BF16),
            *[pltpu.VMEM(w.shape, BF16) for w in arrays[:3]],
            pltpu.VMEM((t, d), BF16),
            pltpu.VMEM((t, d), BF16),
            pltpu.VMEM((d, t), BF16),
            pltpu.VMEM((d, t), BF16),
            pltpu.VMEM((TF, ff), BF16),
            pltpu.VMEM((t, d), F32),
            *[pltpu.VMEM((d, FB), F32)] * 3,
            *[pltpu.VMEM((pieces, d, FB), BF16)] * 2,
            pltpu.VMEM((layers, 2, ff, d // 2), BF16),
            *[pltpu.VMEM((3, n - 1, per, FB), BF16)] * 2,
            pltpu.VMEM((layers * 2, 2, n - 1, per_d // 2, d // 2), BF16),
            *[pltpu.VMEM(a.shape, F32) for a in arrays[3:]],
            *[pltpu.VMEM(a.shape, BF16) for a in arrays[3:6]],
            pltpu.VMEM((8, 128), F32),
            pltpu.VMEM((n - 1, 8, 128), F32),
            dma((5,)),
            dma((6,)),
            dma((3, 2, n - 1)),
            dma((3, 2, n - 1)),
            dma((layers * 2, 2, n - 1)),
            dma((layers * 2, 2, n - 1)),
            dma((n - 1,)),
            dma((n - 1,)),
            dma((2, n - 1, 3)),
            dma((2, n - 1, 3)),
            dma((9,)),
        ],
        compiler_params=pltpu.CompilerParams(vmem_limit_bytes=67_043_328, collective_id=0, has_side_effects=True),
        name="step",
    )(x, dy, *arrays)


def solution(mesh):
    n = mesh.shape["dp"]
    seq, whole, block = P(("rep", "dp"), None, None), P(None, None, None), P(None, "dp", None)
    return jax.shard_map(
        functools.partial(stepped, n),
        mesh=mesh,
        in_specs=(seq, seq, *[whole] * 3, *[block] * 6),
        out_specs=(*[P("rep", None, None)] * 3, *[P("rep", "dp", None)] * 6),
        check_vma=False,
    )
```

```python
import functools

import jax
import jax.numpy as jnp
from jax import lax
from jax.experimental import pallas as pl
from jax.experimental.pallas import tpu as pltpu
from jax.sharding import PartitionSpec as P

BF16, F32 = jnp.bfloat16, jnp.float32
FB = 256
TF = 512
TB = 1024
SUBS = 4
SETS = 4


def dot(a, b):
    return jnp.dot(a, b, preferred_element_type=F32)


def dot_nt(a, b):
    return lax.dot_general(a, b, (((1,), (1,)), ((), ())), preferred_element_type=F32)


def scale_of(wide):
    return lax.rsqrt(jnp.mean(wide * wide, -1, keepdims=True) + 1e-6)


def sigmoid(g):
    return 0.5 * jnp.tanh(0.5 * g) + 0.5


def forward(ready, x, dy, w, h, a2, a_t, dy_t, hid, da):
    wg, wu, wd = w
    blocks = wg.shape[2] // FB

    def tile(i, _):
        ready(i)
        rows = pl.ds(pl.multiple_of(i * TF, TF), TF)
        wide = x[rows, :].astype(F32)
        a = (wide * scale_of(wide)).astype(BF16)
        for j in range(blocks):
            cols = pl.ds(j * FB, FB)
            gate, up = dot(a, wg[0, :, cols]), dot(a, wu[0, :, cols])
            hid[:, cols] = (gate * sigmoid(gate) * up).astype(BF16)
        out = dot(hid[...], wd[0]).astype(BF16).astype(F32)
        state = (wide + out).astype(BF16)
        h[rows, :] = state
        wide = state.astype(F32)
        n = (wide * scale_of(wide)).astype(BF16)
        a2[rows, :] = n
        a_t[:, rows] = n.T
        dy_t[:, rows] = dy[rows, :].T
        x[rows, :] = a
        da[rows, :] = jnp.zeros((TF, x.shape[1]), F32)
        return 0

    lax.fori_loop(0, x.shape[0] // TF, tile, 0)


def backward_tile(layer, j, i, a_ref, a_t, dy, dy_t, w, acc, da):
    wg, wu, wd = w
    rows = pl.ds(pl.multiple_of(i * TB, TB), TB)
    cols = pl.ds(pl.multiple_of(j * FB, FB), FB)
    hids, dgates, dups = [], [], []
    part = TB // SUBS
    for s in range(SUBS):
        sub = pl.ds(pl.multiple_of(i * TB + s * part, part), part)
        a = a_ref[sub, :]
        gate, up = dot(a, wg[layer, :, cols]), dot(a, wu[layer, :, cols])
        dh = dot_nt(dy[sub, :], wd[layer, cols, :]).astype(BF16).astype(F32)
        sg = sigmoid(gate)
        silu = gate * sg
        hids.append((silu * up).astype(BF16))
        dups.append((dh * silu).astype(BF16))
        dgates.append((dh * up * (sg + silu * (1.0 - sg))).astype(BF16))
    hid, dgate, dup = (jnp.concatenate(t, 0) for t in (hids, dgates, dups))
    acc[0][...] += dot(a_t[:, rows], dgate)
    acc[1][...] += dot(a_t[:, rows], dup)
    acc[2][...] += dot(dy_t[:, rows], hid)
    if da is not None:
        da[rows, :] += dot_nt(dgate, wg[layer, :, cols]) + dot_nt(dup, wu[layer, :, cols])


def between(a1, h, dy, a_t, dy_t, da):
    def tile(i, _):
        rows = pl.ds(pl.multiple_of(i * TF, TF), TF)
        wide = h[rows, :].astype(F32)
        by_a = da[rows, :].astype(BF16).astype(F32)
        scale = scale_of(wide)
        inner = jnp.mean(by_a * wide, -1, keepdims=True)
        by_h = scale * by_a - wide * (scale * scale * scale * inner)
        total = (dy[rows, :].astype(F32) + by_h.astype(BF16).astype(F32)).astype(BF16)
        dy[rows, :] = total
        dy_t[:, rows] = total.T
        a_t[:, rows] = a1[rows, :].T
        return 0

    lax.fori_loop(0, h.shape[0] // TF, tile, 0)


def exchanged(me, n):
    return lax.rem(me + 1, n), lax.rem(me + n - 1, n)


def remote(src, dst, send, recv, to):
    return pltpu.make_async_remote_copy(
        src_ref=src, dst_ref=dst, send_sem=send, recv_sem=recv, device_id={"dp": to}, device_id_type=pl.DeviceIdType.MESH
    )


class Chain:
    def __init__(self, terms, slots, send, recv, long, rows, me, n):
        self.terms, self.slots, self.send, self.recv, self.long = terms, slots, send, recv, long
        self.rows, self.me, self.n = rows, me, n

    def hops(self, way):
        return self.n // 2 - (way != self.long)

    def chunk(self, far):
        stride, first, size = self.rows
        at = lax.rem(self.me + self.n + far, self.n)
        return pl.ds(pl.multiple_of(at * stride, size) + first, size)

    def going(self, way, hop):
        left = self.hops(way) - hop
        return self.chunk(left if way == 0 else -left)

    def slot(self, way, hop):
        return hop + (way != self.long) * (self.n // 2)

    def copy(self, way, hop):
        k = self.slot(way, hop)
        return remote(
            self.terms.at[self.going(way, hop), :], self.slots.at[k], self.send.at[k], self.recv.at[k], exchanged(self.me, self.n)[way]
        )

    def step(self, s):
        for way in range(2):
            if 0 < s <= self.hops(way):
                self.copy(way, s - 1).wait()
            if s < self.hops(way):
                if s:
                    self.add(self.going(way, s), self.slot(way, s - 1))
                self.copy(way, s).start()
        if s == self.n // 2:
            self.add(self.chunk(0), *(self.slot(way, self.hops(way) - 1) for way in range(2)))

    def add(self, at, *slots):
        total = self.terms[at, :].astype(F32)
        for k in slots:
            total += self.slots[k].astype(F32)
        self.terms[at, :] = total.astype(BF16)


def kernel(n, x_in, dy_in, wg_in, wu_in, wd_in, mg_in, mu_in, md_in, vg_in, vu_in, vd_in,
           og, ou, od, mg_out, mu_out, md_out, vg_out, vu_out, vd_out,
           x, dy, wg, wu, wd, h, a2, a_t, dy_t, hid, da, ag, au, ad,
           tg, tu, td, slot_gu, slot_d, mg, mu, md, vg, vu, vd, ng, nu, nd, mine, others,
           sems, xsems, msems, rs_send, rs_recv, rd_send, rd_recv, sq_send, sq_recv, ag_send, ag_recv, osems):
    me = lax.axis_index("dp")
    layers, d, ff = wg.shape
    blocks = ff // FB
    ticks = n // 2
    pieces = layers * blocks
    first = [
        pltpu.make_async_copy(src.at[layer], dst.at[layer], sems.at[k, layer])
        for layer in range(layers)
        for k, (src, dst) in enumerate(((wg_in, wg), (wu_in, wu), (wd_in, wd)))
    ]

    def tokens(i):
        rows = pl.ds(pl.multiple_of(i * TF, TF), TF)
        return [pltpu.make_async_copy(src.at[0, rows, :], dst.at[rows, :], xsems.at[k, i]) for k, (src, dst) in enumerate(((x_in, x), (dy_in, dy)))]

    tiles = x.shape[0] // TF
    for c in first[:3] + [c for i in range(tiles) for c in tokens(i)] + first[3:]:
        c.start()
    moments = (mg, mu, md, vg, vu, vd)
    later = [
        pltpu.make_async_copy(src, dst, msems.at[k])
        for k, (src, dst) in enumerate(zip((mg_in, mu_in, md_in, vg_in, vu_in, vd_in), moments, strict=True))
    ]
    for c in later:
        c.start()
    barrier = pltpu.get_barrier_semaphore()
    for off in range(1, n):
        pl.semaphore_signal(barrier, 1, device_id={"dp": lax.rem(me + off, n)}, device_id_type=pl.DeviceIdType.MESH)
    for c in first[:3]:
        c.wait()
    w, acc = (wg, wu, wd), (ag, au, ad)

    def ready(i):
        for c in tokens(i):
            c.wait()

    forward(ready, x, dy, w, h, a2, a_t, dy_t, hid, da)
    for c in first[3:]:
        c.wait()
    pl.semaphore_wait(barrier, n - 1)

    per, per_d = d // n, ff // n
    half = per_d // 2

    def piece(p, s):
        k = lax.rem(p, SETS)
        for which, terms in enumerate((tg, tu)):
            Chain(terms.at[p], slot_gu.at[k, which], rs_send.at[k, which], rs_recv.at[k, which], which, (per, 0, per), me, n).step(s)

    def piece_d(layer, part, s):
        k = layer * 2 + part
        for which in range(2):
            rows = (per_d, part * half, half)
            Chain(td.at[layer, which], slot_d.at[k, which], rd_send.at[k, which], rd_recv.at[k, which], which, rows, me, n).step(s)

    def at_tick(i, tick, p, back, s):
        @pl.when(jnp.logical_and(i == tick, jnp.logical_and(p >= back, p < pieces + back)))
        def _():
            piece(p - back, s)

    def tick(p, i):
        at_tick(i, 0, p, 1, 0)
        at_tick(i, 1, p, 2, 2)
        at_tick(i, 1, p, 3, 4)
        at_tick(i, 2, p, 1, 1)
        at_tick(i, 3, p, 2, 3)

    def tick_d(k):
        for s in range(n // 2 + 1):
            for part in range(2):

                @pl.when(k == 4 * s + 2 * part)
                def _(s=s, part=part):
                    piece_d(1, part, s)

    def backward(layer, first, a_ref, da):
        def block(j, _):
            p = first + j
            for to in acc:
                to[...] = jnp.zeros_like(to)

            def tile(i, _):
                tick(p, i)
                if first:
                    tick_d(j * ticks + i)
                backward_tile(layer, j, i, a_ref, a_t, dy, dy_t, w, acc, da)
                return 0

            lax.fori_loop(0, ticks, tile, 0)
            tg[p] = ag[...].astype(BF16)
            tu[p] = au[...].astype(BF16)
            rows = pl.ds(pl.multiple_of(j * FB, FB), FB)
            by_down = ad[...].astype(BF16).T
            td[layer, 0, rows, :] = by_down[:, : d // 2]
            td[layer, 1, rows, :] = by_down[:, d // 2 :]
            return 0

        lax.fori_loop(0, blocks, block, 0)

    backward(1, 0, a2, da)
    between(x, h, dy, a_t, dy_t, da)
    backward(0, blocks, x, None)

    end = pieces - 1
    for s in range(n // 2 + 1):
        piece(end, s)
        for part in range(2):
            piece_d(0, part, s)
        if s == 0:
            piece(end - 1, 2)
            piece(end - 2, 4)
        elif s < 3:
            piece(end - 1, s + 2)

    own, own_d = pl.ds(pl.multiple_of(me * per, per), per), pl.ds(pl.multiple_of(me * per_d, per_d), per_d)
    total = jnp.zeros((8, 128), F32)

    def squares(t):
        t = t.astype(F32)
        return jnp.sum(t * t)

    local = jnp.float32(0)
    for p in range(pieces):
        local += squares(tg[p, own, :]) + squares(tu[p, own, :])
    for layer in range(layers):
        for way in range(2):
            local += squares(td[layer, way, own_d, :])
    mine[...] = total + local
    sent = [remote(mine, others.at[k - 1], sq_send.at[k - 1], sq_recv.at[k - 1], lax.rem(me + k, n)) for k in range(1, n)]
    for c in sent:
        c.start()
    for c in later:
        c.wait()
    for c in sent:
        c.wait()
    summed = mine[...]
    for k in range(n - 1):
        summed = summed + others[k]
    count = layers * d * ff * 3
    factor = jnp.minimum(1.0, 0.5 * lax.rsqrt(summed[0:1, 0:1] / count + 1e-30))

    def adamw(w_own, m_at, v_at, g, new):
        g = g.astype(F32) * factor
        m_ = 0.9 * m_at[...] + 0.1 * g
        v_ = 0.95 * v_at[...] + 0.05 * g * g
        m_at[...] = m_
        v_at[...] = v_
        w_own = w_own.astype(F32)
        new[...] = (w_own - 0.02 * (m_ * lax.rsqrt(v_ + 1e-8) + 0.1 * w_own)).astype(BF16)

    outs, news, owns = (og, ou, od), (ng, nu, nd), (own, own, own_d)

    def gather(kind, layer, way, hop):
        far = lax.rem(me + n - hop, n) if way == 0 else lax.rem(me + hop, n)
        size = per_d if kind == 2 else per
        rows = outs[kind].at[layer, pl.ds(pl.multiple_of(far * size, size), size), :]
        k = hop + (way != layer % 2) * (n // 2)
        src = rows if hop else news[kind].at[layer]
        return remote(src, rows, ag_send.at[layer, kind, k], ag_recv.at[layer, kind, k], exchanged(me, n)[way])

    def hops(layer, way):
        return n // 2 - (way != layer % 2)

    finals = []
    for kind in range(3):
        for layer in range(layers):
            if kind < 2:
                for j in range(blocks):
                    cols = pl.ds(j * FB, FB)
                    adamw(
                        w[kind][layer, own, cols],
                        (mg, mu)[kind].at[layer, :, cols],
                        (vg, vu)[kind].at[layer, :, cols],
                        (tg, tu)[kind][(layers - 1 - layer) * blocks + j, own, :],
                        news[kind].at[layer, :, cols],
                    )
            else:
                for way in range(2):
                    cols = pl.ds(way * (d // 2), d // 2)
                    adamw(wd[layer, own_d, cols], md.at[layer, :, cols], vd.at[layer, :, cols], td[layer, way, own_d, :], nd.at[layer, :, cols])
            for way in range(2):
                gather(kind, layer, way, 0).start()
        finals.append(pltpu.make_async_copy(news[kind], outs[kind].at[:, owns[kind], :], osems.at[kind]))
        finals.append(pltpu.make_async_copy(moments[kind], (mg_out, mu_out, md_out)[kind], osems.at[3 + kind]))
        finals.append(pltpu.make_async_copy(moments[3 + kind], (vg_out, vu_out, vd_out)[kind], osems.at[6 + kind]))
        for c in finals[-3:]:
            c.start()
    for hop in range(1, n // 2 + 1):
        for kind in range(3):
            for layer in range(layers):
                for way in range(2):
                    if hop <= hops(layer, way):
                        gather(kind, layer, way, hop - 1).wait()
                    if hop < hops(layer, way):
                        gather(kind, layer, way, hop).start()
    for c in finals:
        c.wait()


def stepped(n, x, dy, *arrays):
    _, t, d = x.shape
    wg, _, wd = arrays[:3]
    layers, _, ff = wg.shape
    per, per_d = d // n, ff // n
    pieces = layers * (ff // FB)
    any_ = pl.BlockSpec(memory_space=pl.ANY)
    dma = pltpu.SemaphoreType.DMA
    return pl.pallas_call(
        functools.partial(kernel, n),
        out_shape=[jax.ShapeDtypeStruct(a.shape, a.dtype) for a in arrays],
        in_specs=[any_] * 11,
        out_specs=[any_] * 9,
        scratch_shapes=[
            pltpu.VMEM((t, d), BF16),
            pltpu.VMEM((t, d), BF16),
            *[pltpu.VMEM(w.shape, BF16) for w in arrays[:3]],
            pltpu.VMEM((t, d), BF16),
            pltpu.VMEM((t, d), BF16),
            pltpu.VMEM((d, t), BF16),
            pltpu.VMEM((d, t), BF16),
            pltpu.VMEM((TF, ff), BF16),
            pltpu.VMEM((t, d), F32),
            *[pltpu.VMEM((d, FB), F32)] * 3,
            *[pltpu.VMEM((pieces, d, FB), BF16)] * 2,
            pltpu.VMEM((layers, 2, ff, d // 2), BF16),
            pltpu.VMEM((SETS, 2, n - 1, per, FB), BF16),
            pltpu.VMEM((layers * 2, 2, n - 1, per_d // 2, d // 2), BF16),
            *[pltpu.VMEM(a.shape, F32) for a in arrays[3:]],
            *[pltpu.VMEM(a.shape, BF16) for a in arrays[3:6]],
            pltpu.VMEM((8, 128), F32),
            pltpu.VMEM((n - 1, 8, 128), F32),
            dma((3, layers)),
            dma((2, t // TF)),
            dma((6,)),
            dma((SETS, 2, n - 1)),
            dma((SETS, 2, n - 1)),
            dma((layers * 2, 2, n - 1)),
            dma((layers * 2, 2, n - 1)),
            dma((n - 1,)),
            dma((n - 1,)),
            dma((layers, 3, n - 1)),
            dma((layers, 3, n - 1)),
            dma((9,)),
        ],
        compiler_params=pltpu.CompilerParams(vmem_limit_bytes=67_043_328, collective_id=0, has_side_effects=True),
        name="step",
    )(x, dy, *arrays)


def handed_over(*refs):
    count = len(refs) // 2
    writes = [pltpu.make_async_copy(refs[k], refs[count + k], refs[-1].at[k]) for k in range(count)]
    for c in writes:
        c.start()
    for c in writes:
        c.wait()


def both(n, *arrays):
    results = stepped(n, *arrays)
    parts = len(results)
    return pl.pallas_call(
        handed_over,
        out_shape=[jax.ShapeDtypeStruct(r.shape, r.dtype) for r in results],
        in_specs=[pl.BlockSpec(memory_space=pltpu.VMEM)] * parts,
        out_specs=[pl.BlockSpec(memory_space=pl.ANY)] * parts,
        scratch_shapes=[pltpu.SemaphoreType.DMA((parts,))],
        compiler_params=pltpu.CompilerParams(vmem_limit_bytes=32_000_000),
        name="hand_over",
    )(*results)


def solution(mesh):
    n = mesh.shape["dp"]
    seq, whole, block = P(("rep", "dp"), None, None), P(None, None, None), P(None, "dp", None)
    return jax.shard_map(
        functools.partial(both, n),
        mesh=mesh,
        in_specs=(seq, seq, *[whole] * 3, *[block] * 6),
        out_specs=(*[P("rep", None, None)] * 3, *[P("rep", "dp", None)] * 6),
        check_vma=False,
    )
```

```python
import functools

import jax
import jax.numpy as jnp
from jax import lax
from jax.experimental import pallas as pl
from jax.experimental.pallas import tpu as pltpu
from jax.sharding import PartitionSpec as P

BF16, F32 = jnp.bfloat16, jnp.float32
FB = 256
TF = 512
TB = 1024
SUBS = 4
SETS = 4


def dot(a, b):
    return jnp.dot(a, b, preferred_element_type=F32)


def dot_nt(a, b):
    return lax.dot_general(a, b, (((1,), (1,)), ((), ())), preferred_element_type=F32)


def scale_of(wide):
    return lax.rsqrt(jnp.mean(wide * wide, -1, keepdims=True) + 1e-6)


def sigmoid(g):
    return 0.5 * jnp.tanh(0.5 * g) + 0.5


def grouped(t, n):
    own = t.shape[1] // n
    size = FB // n
    return jnp.concatenate([t[:, own * k + size * j : own * k + size * (j + 1)] for j in range(own // size) for k in range(n)], 1)


def ungrouped(blocks, n):
    size = FB // n
    return jnp.concatenate([t[:, size * k : size * (k + 1)] for k in range(n) for t in blocks], 1)


def forward(n, wg0, wu0, ready, x, dy, w, h, a2, a_t, dy_t, hid, da):
    wg, wu, wd = w
    blocks = wg.shape[2] // FB
    share = wg.shape[1] // (x.shape[0] // TF)

    def tile(i, _):
        ready(i)
        rows = pl.ds(pl.multiple_of(i * TF, TF), TF)
        wide = x[rows, :].astype(F32)
        a = (wide * scale_of(wide)).astype(BF16)
        for j in range(blocks):
            cols = pl.ds(j * FB, FB)
            gate, up = dot(a, wg[0, :, cols]), dot(a, wu[0, :, cols])
            hid[:, cols] = (gate * sigmoid(gate) * up).astype(BF16)
        out = dot(hid[...], wd[0]).astype(BF16).astype(F32)
        state = (wide + out).astype(BF16)
        h[rows, :] = state
        wide = state.astype(F32)
        normed = (wide * scale_of(wide)).astype(BF16)
        a2[rows, :] = normed
        a_t[:, rows] = normed.T
        dy_t[:, rows] = dy[rows, :].T
        x[rows, :] = a
        da[rows, :] = jnp.zeros((TF, x.shape[1]), F32)
        some = pl.ds(pl.multiple_of(i * share, share), share)
        for natural, new in zip((wg, wu), (wg0, wu0), strict=True):
            new[some, :] = grouped(natural[0, some, :], n)
            natural[1, some, :] = grouped(natural[1, some, :], n)
        return 0

    lax.fori_loop(0, x.shape[0] // TF, tile, 0)


def backward_tile(j, i, a_ref, a_t, dy, dy_t, w, acc, da):
    wg, wu, wd = w
    rows = pl.ds(pl.multiple_of(i * TB, TB), TB)
    cols = pl.ds(pl.multiple_of(j * FB, FB), FB)
    hids, dgates, dups = [], [], []
    part = TB // SUBS
    for s in range(SUBS):
        sub = pl.ds(pl.multiple_of(i * TB + s * part, part), part)
        a = a_ref[sub, :]
        gate, up = dot(a, wg[:, cols]), dot(a, wu[:, cols])
        dh = dot_nt(dy[sub, :], wd[cols, :]).astype(BF16).astype(F32)
        sg = sigmoid(gate)
        silu = gate * sg
        hids.append((silu * up).astype(BF16))
        dups.append((dh * silu).astype(BF16))
        dgates.append((dh * up * (sg + silu * (1.0 - sg))).astype(BF16))
    hid, dgate, dup = (jnp.concatenate(t, 0) for t in (hids, dgates, dups))
    acc[0][...] += dot(a_t[:, rows], dgate)
    acc[1][...] += dot(a_t[:, rows], dup)
    acc[2][...] += dot(dy_t[:, rows], hid)
    if da is not None:
        da[rows, :] += dot_nt(dgate, wg[:, cols]) + dot_nt(dup, wu[:, cols])


def between(i, a1, h, dy, a_t, dy_t, da):
    for part in range(TB // TF):
        rows = pl.ds(pl.multiple_of(i * TB + part * TF, TF), TF)
        wide = h[rows, :].astype(F32)
        by_a = da[rows, :].astype(BF16).astype(F32)
        scale = scale_of(wide)
        inner = jnp.mean(by_a * wide, -1, keepdims=True)
        by_h = scale * by_a - wide * (scale * scale * scale * inner)
        total = (dy[rows, :].astype(F32) + by_h.astype(BF16).astype(F32)).astype(BF16)
        dy[rows, :] = total
        dy_t[:, rows] = total.T
        a_t[:, rows] = a1[rows, :].T


def exchanged(me, n):
    return lax.rem(me + 1, n), lax.rem(me + n - 1, n)


def remote(src, dst, send, recv, to):
    return pltpu.make_async_remote_copy(
        src_ref=src, dst_ref=dst, send_sem=send, recv_sem=recv, device_id={"dp": to}, device_id_type=pl.DeviceIdType.MESH
    )


class Chain:
    def __init__(self, terms, slots, send, recv, long, me, n):
        self.terms, self.slots, self.send, self.recv, self.long, self.me, self.n = terms, slots, send, recv, long, me, n

    def hops(self, way):
        return self.n // 2 - (way != self.long)

    def chunk(self, far):
        return lax.rem(self.me + self.n + far, self.n)

    def going(self, way, hop):
        left = self.hops(way) - hop
        return self.chunk(left if way == 0 else -left)

    def slot(self, way, hop):
        return hop + (way != self.long) * (self.n // 2)

    def copy(self, way, hop):
        k = self.slot(way, hop)
        return remote(
            self.terms.at[self.going(way, hop)], self.slots.at[k], self.send.at[k], self.recv.at[k], exchanged(self.me, self.n)[way]
        )

    def step(self, s):
        for way in range(2):
            if 0 < s <= self.hops(way):
                self.copy(way, s - 1).wait()
            if s < self.hops(way):
                if s:
                    self.add(self.going(way, s), self.slot(way, s - 1))
                self.copy(way, s).start()
        if s == self.n // 2:
            self.add(self.chunk(0), *(self.slot(way, self.hops(way) - 1) for way in range(2)))

    def add(self, at, *slots):
        total = self.terms[at].astype(F32)
        for k in slots:
            total += self.slots[k].astype(F32)
        self.terms[at] = total.astype(BF16)


def kernel(n, x_in, dy_in, wg_in, wu_in, wd_in, mg_in, mu_in, md_in, vg_in, vu_in, vd_in,
           og, ou, od, mg_out, mu_out, md_out, vg_out, vu_out, vd_out,
           x, dy, wg, wu, wd, h, a2, a_t, dy_t, hid, da, ag, au, ad,
           wg0, wu0, t0, t1, slots, mg, mu, md, vg, vu, vd, ng, nu, nd, mine, others,
           sems, xsems, gsems, msems, rs_send, rs_recv, sq_send, sq_recv, ag_send, ag_recv, osems):
    me = lax.axis_index("dp")
    layers, d, ff = wg.shape
    blocks = ff // FB
    ticks = n // 2
    per, per_d, part_d = d // n, ff // n, FB // n
    pieces = layers * blocks
    def load(which, layer):
        src, dst = ((wg_in, wg), (wu_in, wu), (wd_in, wd))[which]
        return pltpu.make_async_copy(src.at[layer], dst.at[layer], sems.at[which, layer])

    def load_grouped(layer):
        def one(k, _):
            to, j = k // blocks, lax.rem(k, blocks)
            src = pl.ds(pl.multiple_of(to * per_d + j * part_d, part_d), part_d)
            dst = pl.ds(pl.multiple_of(j * FB + to * part_d, part_d), part_d)
            pltpu.make_async_copy(wd_in.at[layer, src, :], wd.at[layer, dst, :], gsems.at[layer]).start()
            return 0

        lax.fori_loop(0, n * blocks, one, 0)

    def grouped_loaded(layer):
        pltpu.make_async_copy(wd_in.at[layer], wd.at[layer], gsems.at[layer]).wait()

    def tokens(i):
        rows = pl.ds(pl.multiple_of(i * TF, TF), TF)
        return [pltpu.make_async_copy(src.at[0, rows, :], dst.at[rows, :], xsems.at[k, i]) for k, (src, dst) in enumerate(((x_in, x), (dy_in, dy)))]

    tiles = x.shape[0] // TF
    before = [load(0, 0), load(1, 0), load(2, 0), load(0, 1), load(1, 1)]
    for c in before[:3] + tokens(0) + before[3:] + [c for i in range(1, tiles) for c in tokens(i)]:
        c.start()
    load_grouped(1)
    moments = (mg, mu, md, vg, vu, vd)
    later = [
        pltpu.make_async_copy(src, dst, msems.at[k])
        for k, (src, dst) in enumerate(zip((mg_in, mu_in, md_in, vg_in, vu_in, vd_in), moments, strict=True))
    ]
    own, own_d = pl.ds(pl.multiple_of(me * per, per), per), pl.ds(pl.multiple_of(me * per_d, per_d), per_d)
    owned = ((wg_in, own, ng), (wu_in, own, nu), (wd_in, own_d, nd))
    later += [pltpu.make_async_copy(src.at[:, at, :], dst, msems.at[6 + k]) for k, (src, at, dst) in enumerate(owned)]
    for c in later:
        c.start()
    barrier = pltpu.get_barrier_semaphore()
    for off in range(1, n):
        pl.semaphore_signal(barrier, 1, device_id={"dp": lax.rem(me + off, n)}, device_id_type=pl.DeviceIdType.MESH)
    for c in before:
        c.wait()
    w, acc = (wg, wu, wd), (ag, au, ad)

    def ready(i):
        for c in tokens(i):
            c.wait()

    forward(n, wg0, wu0, ready, x, dy, w, h, a2, a_t, dy_t, hid, da)
    load_grouped(0)
    grouped_loaded(1)
    pl.semaphore_wait(barrier, n - 1)


    def piece(p, s):
        k = lax.rem(p, SETS)
        for which, terms in enumerate((t0, t1)):
            Chain(terms.at[p], slots.at[k, which], rs_send.at[k, which], rs_recv.at[k, which], which, me, n).step(s)

    def at_tick(i, tick, p, back, s):
        @pl.when(jnp.logical_and(i == tick, jnp.logical_and(p >= back, p < pieces + back)))
        def _():
            piece(p - back, s)

    def tick(p, i):
        at_tick(i, 0, p, 1, 0)
        at_tick(i, 1, p, 2, 2)
        at_tick(i, 1, p, 3, 4)
        at_tick(i, 2, p, 1, 1)
        at_tick(i, 3, p, 2, 3)

    da_all = da

    def backward(layer, first, a_ref, da):
        of_layer = (wg0, wu0, wd.at[0]) if layer == 0 else (wg.at[1], wu.at[1], wd.at[1])

        def block(j, _, fresh=False):
            p = first + j
            for to in acc:
                to[...] = jnp.zeros_like(to)

            def tile(i, _):
                tick(p, i)
                if fresh:
                    between(i, x, h, dy, a_t, dy_t, da_all)
                backward_tile(j, i, a_ref, a_t, dy, dy_t, of_layer, acc, da)
                return 0

            lax.fori_loop(0, ticks, tile, 0)
            by_down = ad[...].astype(BF16).T
            for terms, of_in, of_down in ((t0, ag, by_down[:, : d // 2]), (t1, au, by_down[:, d // 2 :])):
                terms[p, :, :per, :] = of_in[...].astype(BF16).reshape(n, per, FB)
                terms[p, :, per:, :] = of_down.reshape(n, part_d, FB)
            return 0

        if layer == 0:
            block(0, 0, True)
        lax.fori_loop(1 if layer == 0 else 0, blocks, block, 0)

    backward(1, 0, a2, da)
    grouped_loaded(0)
    backward(0, blocks, x, None)

    def squares(p):
        return sum(jnp.sum(t * t) for t in (terms[p, me].astype(F32) for terms in (t0, t1)))

    end = pieces - 1
    local = jnp.float32(0)
    for s in range(n // 2 + 1):
        piece(end, s)
        if s == 0:
            piece(end - 1, 2)
            piece(end - 2, 4)
        elif s < 3:
            piece(end - 1, s + 2)
        elif s == 3:
            local += sum(squares(p) for p in range(end))

    local += squares(end)
    total = jnp.zeros((8, 128), F32)
    mine[...] = total + local
    sent = [remote(mine, others.at[k - 1], sq_send.at[k - 1], sq_recv.at[k - 1], lax.rem(me + k, n)) for k in range(1, n)]
    for c in sent:
        c.start()
    for c in later:
        c.wait()
    for c in sent:
        c.wait()
    summed = mine[...]
    for k in range(n - 1):
        summed = summed + others[k]
    count = layers * d * ff * 3
    factor = jnp.minimum(1.0, 0.5 * lax.rsqrt(summed[0:1, 0:1] / count + 1e-30))

    def adamw(m_at, v_at, g, new):
        g = g.astype(F32) * factor
        m_ = 0.9 * m_at[...] + 0.1 * g
        v_ = 0.95 * v_at[...] + 0.05 * g * g
        m_at[...] = m_
        v_at[...] = v_
        old = new[...].astype(F32)
        new[...] = (old - 0.02 * (m_ * lax.rsqrt(v_ + 1e-8) + 0.1 * old)).astype(BF16)

    outs, news, owns = (og, ou, od), (ng, nu, nd), (own, own, own_d)

    def gather(kind, layer, way, hop):
        far = lax.rem(me + n - hop, n) if way == 0 else lax.rem(me + hop, n)
        size = per_d if kind == 2 else per
        rows = outs[kind].at[layer, pl.ds(pl.multiple_of(far * size, size), size), :]
        k = hop + (way != layer % 2) * (n // 2)
        src = rows if hop else news[kind].at[layer]
        return remote(src, rows, ag_send.at[layer, kind, k], ag_recv.at[layer, kind, k], exchanged(me, n)[way])

    def hops(layer, way):
        return n // 2 - (way != layer % 2)

    finals = []
    for kind in range(3):
        for layer in range(layers):
            of = range((layers - 1 - layer) * blocks, (layers - layer) * blocks)
            m_at, v_at, new = (t.at[layer] for t in (moments[kind], moments[3 + kind], news[kind]))
            if kind < 2:
                adamw(m_at, v_at, ungrouped([(t0, t1)[kind][p, me, :per, :] for p in of], n), new)
            else:
                for j, p in enumerate(of):
                    for way in range(2):
                        at = pl.ds(j * part_d, part_d), pl.ds(way * (d // 2), d // 2)
                        adamw(m_at.at[at], v_at.at[at], (t0, t1)[way][p, me, per:, :], new.at[at])
            for way in range(2):
                gather(kind, layer, way, 0).start()
        finals.append(pltpu.make_async_copy(news[kind], outs[kind].at[:, owns[kind], :], osems.at[kind]))
        finals.append(pltpu.make_async_copy(moments[kind], (mg_out, mu_out, md_out)[kind], osems.at[3 + kind]))
        finals.append(pltpu.make_async_copy(moments[3 + kind], (vg_out, vu_out, vd_out)[kind], osems.at[6 + kind]))
        for c in finals[-3:]:
            c.start()
    for hop in range(1, n // 2 + 1):
        for kind in range(3):
            for layer in range(layers):
                for way in range(2):
                    if hop <= hops(layer, way):
                        gather(kind, layer, way, hop - 1).wait()
                    if hop < hops(layer, way):
                        gather(kind, layer, way, hop).start()
    for c in finals:
        c.wait()


def stepped(n, x, dy, *arrays):
    _, t, d = x.shape
    wg, _, wd = arrays[:3]
    layers, _, ff = wg.shape
    per = d // n
    pieces = layers * (ff // FB)
    any_ = pl.BlockSpec(memory_space=pl.ANY)
    dma = pltpu.SemaphoreType.DMA
    return pl.pallas_call(
        functools.partial(kernel, n),
        out_shape=[jax.ShapeDtypeStruct(a.shape, a.dtype) for a in arrays],
        in_specs=[any_] * 11,
        out_specs=[any_] * 9,
        scratch_shapes=[
            pltpu.VMEM((t, d), BF16),
            pltpu.VMEM((t, d), BF16),
            *[pltpu.VMEM(w.shape, BF16) for w in arrays[:3]],
            pltpu.VMEM((t, d), BF16),
            pltpu.VMEM((t, d), BF16),
            pltpu.VMEM((d, t), BF16),
            pltpu.VMEM((d, t), BF16),
            pltpu.VMEM((TF, ff), BF16),
            pltpu.VMEM((t, d), F32),
            *[pltpu.VMEM((d, FB), F32)] * 3,
            *[pltpu.VMEM((d, ff), BF16)] * 2,
            *[pltpu.VMEM((pieces, n, per + FB // n, FB), BF16)] * 2,
            pltpu.VMEM((SETS, 2, n - 1, per + FB // n, FB), BF16),
            *[pltpu.VMEM(a.shape, F32) for a in arrays[3:]],
            *[pltpu.VMEM(a.shape, BF16) for a in arrays[3:6]],
            pltpu.VMEM((8, 128), F32),
            pltpu.VMEM((n - 1, 8, 128), F32),
            dma((3, layers)),
            dma((2, t // TF)),
            dma((layers,)),
            dma((9,)),
            dma((SETS, 2, n - 1)),
            dma((SETS, 2, n - 1)),
            dma((n - 1,)),
            dma((n - 1,)),
            dma((layers, 3, n - 1)),
            dma((layers, 3, n - 1)),
            dma((9,)),
        ],
        compiler_params=pltpu.CompilerParams(vmem_limit_bytes=67_043_328, collective_id=0, has_side_effects=True),
        name="step",
    )(x, dy, *arrays)


def handed_over(*refs):
    count = (len(refs) - 1) // 3
    steps = [(layer, k) for k in range(count) for layer in range(refs[k].shape[0])]
    sems = refs[-1]

    def copy(which, layer, k):
        return pltpu.make_async_copy(
            refs[k + (0, 2)[which] * count].at[layer], refs[k + (2, 1)[which] * count].at[layer], sems.at[which, k, layer]
        )

    for at in steps:
        copy(0, *at).start()
    for at in steps:
        copy(0, *at).wait()
        copy(1, *at).start()
    for at in steps:
        copy(1, *at).wait()


def both(n, *arrays):
    results = stepped(n, *arrays)
    parts = len(results)
    any_ = pl.BlockSpec(memory_space=pl.ANY)
    return pl.pallas_call(
        handed_over,
        out_shape=[jax.ShapeDtypeStruct(r.shape, r.dtype) for r in results],
        in_specs=[any_] * parts,
        out_specs=[any_] * parts,
        scratch_shapes=[*[pltpu.VMEM(r.shape, r.dtype) for r in results], pltpu.SemaphoreType.DMA((2, parts, results[0].shape[0]))],
        compiler_params=pltpu.CompilerParams(vmem_limit_bytes=67_043_328),
        name="hand_over",
    )(*results)


def solution(mesh):
    n = mesh.shape["dp"]
    seq, whole, block = P(("rep", "dp"), None, None), P(None, None, None), P(None, "dp", None)
    return jax.shard_map(
        functools.partial(both, n),
        mesh=mesh,
        in_specs=(seq, seq, *[whole] * 3, *[block] * 6),
        out_specs=(*[P("rep", None, None)] * 3, *[P("rep", "dp", None)] * 6),
        check_vma=False,
    )
```

```python
import functools

import jax
import jax.numpy as jnp
from jax import lax
from jax.experimental import pallas as pl
from jax.experimental.pallas import tpu as pltpu
from jax.sharding import PartitionSpec as P

BF16, F32 = jnp.bfloat16, jnp.float32
FB = 256
TF = 512
TB = 1024
SUBS = 4
SETS = 5


def dot(a, b):
    return jnp.dot(a, b, preferred_element_type=F32)


def dot_nt(a, b):
    return lax.dot_general(a, b, (((1,), (1,)), ((), ())), preferred_element_type=F32)


def scale_of(wide):
    return lax.rsqrt(jnp.mean(wide * wide, -1, keepdims=True) + 1e-6)


def sigmoid(g):
    return 0.5 * jnp.tanh(0.5 * g) + 0.5


def grouped(t, n):
    own = t.shape[1] // n
    size = FB // n
    return jnp.concatenate([t[:, own * k + size * j : own * k + size * (j + 1)] for j in range(own // size) for k in range(n)], 1)


def ungrouped(blocks, n):
    size = FB // n
    return jnp.concatenate([t[:, size * k : size * (k + 1)] for k in range(n) for t in blocks], 1)


def forward(n, ready, x, dy, w, h, a2, a_t, dy_t, hid, da):
    wg, wu, wd = w
    blocks = wg.shape[2] // FB
    share = wg.shape[1] // (x.shape[0] // TF)

    def tile(i, _):
        ready(i)
        rows = pl.ds(pl.multiple_of(i * TF, TF), TF)
        wide = x[rows, :].astype(F32)
        a = (wide * scale_of(wide)).astype(BF16)
        for j in range(blocks):
            cols = pl.ds(j * FB, FB)
            gate, up = dot(a, wg[0, :, cols]), dot(a, wu[0, :, cols])
            hid[:, cols] = (gate * sigmoid(gate) * up).astype(BF16)
        out = dot(hid[...], wd[0]).astype(BF16).astype(F32)
        state = (wide + out).astype(BF16)
        h[rows, :] = state
        wide = state.astype(F32)
        normed = (wide * scale_of(wide)).astype(BF16)
        a2[rows, :] = normed
        a_t[:, rows] = normed.T
        dy_t[:, rows] = dy[rows, :].T
        x[rows, :] = a
        da[rows, :] = jnp.zeros((TF, x.shape[1]), F32)
        some = pl.ds(pl.multiple_of(i * share, share), share)
        for natural in (wg, wu):
            natural[1, some, :] = grouped(natural[1, some, :], n)
        return 0

    lax.fori_loop(0, x.shape[0] // TF, tile, 0)


def backward_tile(j, i, a_ref, a_t, dy, dy_t, w, acc, da):
    wg, wu, wd = w
    rows = pl.ds(pl.multiple_of(i * TB, TB), TB)
    cols = pl.ds(pl.multiple_of(j * FB, FB), FB)
    hids, dgates, dups = [], [], []
    part = TB // SUBS
    for s in range(SUBS):
        sub = pl.ds(pl.multiple_of(i * TB + s * part, part), part)
        a = a_ref[sub, :]
        gate, up = dot(a, wg[:, cols]), dot(a, wu[:, cols])
        dh = dot_nt(dy[sub, :], wd[cols, :]).astype(BF16).astype(F32)
        sg = sigmoid(gate)
        silu = gate * sg
        hids.append((silu * up).astype(BF16))
        dups.append((dh * silu).astype(BF16))
        dgates.append((dh * up * (sg + silu * (1.0 - sg))).astype(BF16))
    hid, dgate, dup = (jnp.concatenate(t, 0) for t in (hids, dgates, dups))
    acc[0][...] += dot(a_t[:, rows], dgate)
    acc[1][...] += dot(a_t[:, rows], dup)
    acc[2][...] += dot(dy_t[:, rows], hid)
    if da is not None:
        da[rows, :] += dot_nt(dgate, wg[:, cols]) + dot_nt(dup, wu[:, cols])


def between(i, a1, h, dy, a_t, dy_t, da):
    for part in range(TB // TF):
        rows = pl.ds(pl.multiple_of(i * TB + part * TF, TF), TF)
        wide = h[rows, :].astype(F32)
        by_a = da[rows, :].astype(BF16).astype(F32)
        scale = scale_of(wide)
        inner = jnp.mean(by_a * wide, -1, keepdims=True)
        by_h = scale * by_a - wide * (scale * scale * scale * inner)
        total = (dy[rows, :].astype(F32) + by_h.astype(BF16).astype(F32)).astype(BF16)
        dy[rows, :] = total
        dy_t[:, rows] = total.T
        a_t[:, rows] = a1[rows, :].T


def exchanged(me, n):
    return lax.rem(me + 1, n), lax.rem(me + n - 1, n)


def remote(src, dst, send, recv, to):
    return pltpu.make_async_remote_copy(
        src_ref=src, dst_ref=dst, send_sem=send, recv_sem=recv, device_id={"dp": to}, device_id_type=pl.DeviceIdType.MESH
    )


class Chain:
    def __init__(self, terms, slots, send, recv, long, me, n):
        self.terms, self.slots, self.send, self.recv, self.long, self.me, self.n = terms, slots, send, recv, long, me, n

    def hops(self, way):
        return self.n // 2 - (way != self.long)

    def chunk(self, far):
        return lax.rem(self.me + self.n + far, self.n)

    def going(self, way, hop):
        left = self.hops(way) - hop
        return self.chunk(left if way == 0 else -left)

    def slot(self, way, hop):
        return hop + (way != self.long) * (self.n // 2)

    def copy(self, way, hop):
        k = self.slot(way, hop)
        return remote(
            self.terms.at[self.going(way, hop)], self.slots.at[k], self.send.at[k], self.recv.at[k], exchanged(self.me, self.n)[way]
        )

    def step(self, s):
        for way in range(2):
            if 0 < s <= self.hops(way):
                self.copy(way, s - 1).wait()
            if s < self.hops(way):
                if s:
                    self.add(self.going(way, s), self.slot(way, s - 1))
                self.copy(way, s).start()
        if s == self.n // 2:
            self.add(self.chunk(0), *(self.slot(way, self.hops(way) - 1) for way in range(2)))

    def add(self, at, *slots):
        total = self.terms[at].astype(F32)
        for k in slots:
            total += self.slots[k].astype(F32)
        self.terms[at] = total.astype(BF16)


def kernel(n, x_in, dy_in, wg_in, wu_in, wd_in, mg_in, mu_in, md_in, vg_in, vu_in, vd_in,
           og, ou, od, mg_out, mu_out, md_out, vg_out, vu_out, vd_out,
           x, dy, wg, wu, wd, h, a2, a_t, dy_t, hid, da, ag, au, ad,
           wg0, wu0, t0, t1, slots, mg, mu, md, vg, vu, vd, ng, nu, nd, mine, others,
           sems, xsems, gsems, msems, rs_send, rs_recv, sq_send, sq_recv, ag_send, ag_recv, osems):
    me = lax.axis_index("dp")
    layers, d, ff = wg.shape
    blocks = ff // FB
    ticks = n // 2
    per, per_d, part_d = d // n, ff // n, FB // n
    pieces = layers * blocks
    def load(which, layer):
        src, dst = ((wg_in, wg), (wu_in, wu), (wd_in, wd))[which]
        return pltpu.make_async_copy(src.at[layer], dst.at[layer], sems.at[which, layer])

    def load_grouped(layer):
        def one(k, _):
            to, j = k // blocks, lax.rem(k, blocks)
            src = pl.ds(pl.multiple_of(to * per_d + j * part_d, part_d), part_d)
            dst = pl.ds(pl.multiple_of(j * FB + to * part_d, part_d), part_d)
            pltpu.make_async_copy(wd_in.at[layer, src, :], wd.at[layer, dst, :], gsems.at[layer]).start()
            return 0

        lax.fori_loop(0, n * blocks, one, 0)

    def grouped_loaded(layer):
        pltpu.make_async_copy(wd_in.at[layer], wd.at[layer], gsems.at[layer]).wait()

    def tokens(i):
        rows = pl.ds(pl.multiple_of(i * TF, TF), TF)
        return [pltpu.make_async_copy(src.at[0, rows, :], dst.at[rows, :], xsems.at[k, i]) for k, (src, dst) in enumerate(((x_in, x), (dy_in, dy)))]

    tiles = x.shape[0] // TF
    before = [load(0, 0), load(1, 0), load(2, 0), load(0, 1), load(1, 1)]
    for c in before[:3] + tokens(0) + before[3:] + [c for i in range(1, tiles) for c in tokens(i)]:
        c.start()
    load_grouped(1)
    moments = (mg, mu, md, vg, vu, vd)
    later = [
        pltpu.make_async_copy(src, dst, msems.at[k])
        for k, (src, dst) in enumerate(zip((mg_in, mu_in, md_in, vg_in, vu_in, vd_in), moments, strict=True))
    ]
    own, own_d = pl.ds(pl.multiple_of(me * per, per), per), pl.ds(pl.multiple_of(me * per_d, per_d), per_d)
    owned = ((wg_in, own, ng), (wu_in, own, nu), (wd_in, own_d, nd))
    later += [pltpu.make_async_copy(src.at[:, at, :], dst, msems.at[6 + k]) for k, (src, at, dst) in enumerate(owned)]
    for c in later:
        c.start()
    barrier = pltpu.get_barrier_semaphore()
    for off in range(1, n):
        pl.semaphore_signal(barrier, 1, device_id={"dp": lax.rem(me + off, n)}, device_id_type=pl.DeviceIdType.MESH)
    for c in before:
        c.wait()
    w, acc = (wg, wu, wd), (ag, au, ad)

    def ready(i):
        for c in tokens(i):
            c.wait()

    forward(n, ready, x, dy, w, h, a2, a_t, dy_t, hid, da)
    load_grouped(0)
    grouped_loaded(1)
    pl.semaphore_wait(barrier, n - 1)


    def piece(p, s):
        k = lax.rem(p, SETS)
        for which, terms in enumerate((t0, t1)):
            Chain(terms.at[p], slots.at[k, which], rs_send.at[k, which], rs_recv.at[k, which], which, me, n).step(s)

    def at_tick(i, tick, p, back, s):
        @pl.when(jnp.logical_and(i == tick, jnp.logical_and(p >= back, p < pieces + back)))
        def _():
            piece(p - back, s)

    def tick(p, i):
        at_tick(i, 0, p, 1, 0)
        at_tick(i, 0, p, 4, 4)
        at_tick(i, 1, p, 3, 3)
        at_tick(i, 2, p, 2, 2)
        at_tick(i, 3, p, 1, 1)

    da_all = da

    def backward(layer, first, a_ref, da):
        of_layer = (wg0, wu0, wd.at[0]) if layer == 0 else (wg.at[1], wu.at[1], wd.at[1])

        def block(j, _, fresh=False):
            p = first + j
            for to in acc:
                to[...] = jnp.zeros_like(to)

            def tile(i, _):
                tick(p, i)
                if fresh:
                    between(i, x, h, dy, a_t, dy_t, da_all)
                backward_tile(j, i, a_ref, a_t, dy, dy_t, of_layer, acc, da)
                return 0

            lax.fori_loop(0, ticks, tile, 0)
            by_down = ad[...].astype(BF16).T
            for terms, of_in, of_down in ((t0, ag, by_down[:, : d // 2]), (t1, au, by_down[:, d // 2 :])):
                terms[p, :, :per, :] = of_in[...].astype(BF16).reshape(n, per, FB)
                terms[p, :, per:, :] = of_down.reshape(n, part_d, FB)
            return 0

        if layer == 0:
            block(0, 0, True)
        lax.fori_loop(1 if layer == 0 else 0, blocks, block, 0)

    backward(1, 0, a2, da)
    grouped_loaded(0)

    def regroup(i, _):
        some = pl.ds(pl.multiple_of(i * per, per), per)
        for natural, new in ((wg, wg0), (wu, wu0)):
            new[some, :] = grouped(natural[0, some, :], n)
        return 0

    lax.fori_loop(0, n, regroup, 0)
    backward(0, blocks, x, None)

    def squares(p):
        return sum(jnp.sum(t * t) for t in (terms[p, me].astype(F32) for terms in (t0, t1)))

    end = pieces - 1
    local = jnp.float32(0)
    for s in range(n // 2 + 1):
        piece(end, s)
        if s < 3:
            for back in range(1, 4 - s):
                piece(end - back, s + 1 + back)
        elif s == 3:
            local += sum(squares(p) for p in range(end))

    local += squares(end)
    total = jnp.zeros((8, 128), F32)
    mine[...] = total + local
    sent = [remote(mine, others.at[k - 1], sq_send.at[k - 1], sq_recv.at[k - 1], lax.rem(me + k, n)) for k in range(1, n)]
    for c in sent:
        c.start()
    for c in later:
        c.wait()
    for c in sent:
        c.wait()
    summed = mine[...]
    for k in range(n - 1):
        summed = summed + others[k]
    count = layers * d * ff * 3
    factor = jnp.minimum(1.0, 0.5 * lax.rsqrt(summed[0:1, 0:1] / count + 1e-30))

    def adamw(m_at, v_at, g, new):
        g = g.astype(F32) * factor
        m_ = 0.9 * m_at[...] + 0.1 * g
        v_ = 0.95 * v_at[...] + 0.05 * g * g
        m_at[...] = m_
        v_at[...] = v_
        old = new[...].astype(F32)
        new[...] = (old - 0.02 * (m_ * lax.rsqrt(v_ + 1e-8) + 0.1 * old)).astype(BF16)

    outs, news, owns = (og, ou, od), (ng, nu, nd), (own, own, own_d)

    def gather(kind, layer, way, hop):
        far = lax.rem(me + n - hop, n) if way == 0 else lax.rem(me + hop, n)
        size = per_d if kind == 2 else per
        rows = outs[kind].at[layer, pl.ds(pl.multiple_of(far * size, size), size), :]
        k = hop + (way != layer % 2) * (n // 2)
        src = rows if hop else news[kind].at[layer]
        return remote(src, rows, ag_send.at[layer, kind, k], ag_recv.at[layer, kind, k], exchanged(me, n)[way])

    def hops(layer, way):
        return n // 2 - (way != layer % 2)

    finals = []
    for kind in range(3):
        for layer in range(layers):
            of = range((layers - 1 - layer) * blocks, (layers - layer) * blocks)
            m_at, v_at, new = (t.at[layer] for t in (moments[kind], moments[3 + kind], news[kind]))
            if kind < 2:
                adamw(m_at, v_at, ungrouped([(t0, t1)[kind][p, me, :per, :] for p in of], n), new)
            else:
                for j, p in enumerate(of):
                    for way in range(2):
                        at = pl.ds(j * part_d, part_d), pl.ds(way * (d // 2), d // 2)
                        adamw(m_at.at[at], v_at.at[at], (t0, t1)[way][p, me, per:, :], new.at[at])
            for way in range(2):
                gather(kind, layer, way, 0).start()
        finals.append(pltpu.make_async_copy(news[kind], outs[kind].at[:, owns[kind], :], osems.at[kind]))
        finals.append(pltpu.make_async_copy(moments[kind], (mg_out, mu_out, md_out)[kind], osems.at[3 + kind]))
        finals.append(pltpu.make_async_copy(moments[3 + kind], (vg_out, vu_out, vd_out)[kind], osems.at[6 + kind]))
        for c in finals[-3:]:
            c.start()
    for hop in range(1, n // 2 + 1):
        for kind in range(3):
            for layer in range(layers):
                for way in range(2):
                    if hop <= hops(layer, way):
                        gather(kind, layer, way, hop - 1).wait()
                    if hop < hops(layer, way):
                        gather(kind, layer, way, hop).start()
    for c in finals:
        c.wait()


def stepped(n, x, dy, *arrays):
    _, t, d = x.shape
    wg, _, wd = arrays[:3]
    layers, _, ff = wg.shape
    per = d // n
    pieces = layers * (ff // FB)
    any_ = pl.BlockSpec(memory_space=pl.ANY)
    dma = pltpu.SemaphoreType.DMA
    return pl.pallas_call(
        functools.partial(kernel, n),
        out_shape=[jax.ShapeDtypeStruct(a.shape, a.dtype) for a in arrays],
        in_specs=[any_] * 11,
        out_specs=[any_] * 9,
        scratch_shapes=[
            pltpu.VMEM((t, d), BF16),
            pltpu.VMEM((t, d), BF16),
            *[pltpu.VMEM(w.shape, BF16) for w in arrays[:3]],
            pltpu.VMEM((t, d), BF16),
            pltpu.VMEM((t, d), BF16),
            pltpu.VMEM((d, t), BF16),
            pltpu.VMEM((d, t), BF16),
            pltpu.VMEM((TF, ff), BF16),
            pltpu.VMEM((t, d), F32),
            *[pltpu.VMEM((d, FB), F32)] * 3,
            *[pltpu.VMEM((d, ff), BF16)] * 2,
            *[pltpu.VMEM((pieces, n, per + FB // n, FB), BF16)] * 2,
            pltpu.VMEM((SETS, 2, n - 1, per + FB // n, FB), BF16),
            *[pltpu.VMEM(a.shape, F32) for a in arrays[3:]],
            *[pltpu.VMEM(a.shape, BF16) for a in arrays[3:6]],
            pltpu.VMEM((8, 128), F32),
            pltpu.VMEM((n - 1, 8, 128), F32),
            dma((3, layers)),
            dma((2, t // TF)),
            dma((layers,)),
            dma((9,)),
            dma((SETS, 2, n - 1)),
            dma((SETS, 2, n - 1)),
            dma((n - 1,)),
            dma((n - 1,)),
            dma((layers, 3, n - 1)),
            dma((layers, 3, n - 1)),
            dma((9,)),
        ],
        compiler_params=pltpu.CompilerParams(vmem_limit_bytes=67_043_328, collective_id=0, has_side_effects=True),
        name="step",
    )(x, dy, *arrays)


def handed_over(*refs):
    count = (len(refs) - 1) // 3
    steps = [(layer, k) for k in range(count) for layer in range(refs[k].shape[0])]
    sems = refs[-1]

    def copy(which, layer, k):
        return pltpu.make_async_copy(
            refs[k + (0, 2)[which] * count].at[layer], refs[k + (2, 1)[which] * count].at[layer], sems.at[which, k, layer]
        )

    for at in steps:
        copy(0, *at).start()
    for at in steps:
        copy(0, *at).wait()
        copy(1, *at).start()
    for at in steps:
        copy(1, *at).wait()


def both(n, *arrays):
    results = stepped(n, *arrays)
    parts = len(results)
    any_ = pl.BlockSpec(memory_space=pl.ANY)
    return pl.pallas_call(
        handed_over,
        out_shape=[jax.ShapeDtypeStruct(r.shape, r.dtype) for r in results],
        in_specs=[any_] * parts,
        out_specs=[any_] * parts,
        scratch_shapes=[*[pltpu.VMEM(r.shape, r.dtype) for r in results], pltpu.SemaphoreType.DMA((2, parts, results[0].shape[0]))],
        compiler_params=pltpu.CompilerParams(vmem_limit_bytes=67_043_328),
        name="hand_over",
    )(*results)


def solution(mesh):
    n = mesh.shape["dp"]
    seq, whole, block = P(("rep", "dp"), None, None), P(None, None, None), P(None, "dp", None)
    return jax.shard_map(
        functools.partial(both, n),
        mesh=mesh,
        in_specs=(seq, seq, *[whole] * 3, *[block] * 6),
        out_specs=(*[P("rep", None, None)] * 3, *[P("rep", "dp", None)] * 6),
        check_vma=False,
    )
```
